32 devices in a mesh: vert: 4 (over y, x), feat: 8 (over z, core).
Axes of the slice: x: 2, y: 2, z: 4, core: 2. Of those that a mesh axis runs over, the one named last changes fastest.
Arguments:
- features: bfloat16 [32768, 256], P('vert', 'feat'), may hold values from -6 to 6
- tiles: bfloat16 [256, 16, 128, 128], P('vert'), may hold values from -0.1875 to 0.1875
- tile_cols: int32 [256, 16], P('vert'), may hold values from 0 to 79
- tile_count: int32 [256], P('vert'), may hold values from 1 to 16, as said below
- send_list: int32 [4, 4, 4], P('vert'), may hold values from 0 to 63
- weight: bfloat16 [256, 256], replicated, may hold values from -0.375 to 0.375
- bias: float32 [256], replicated, may hold values from -3 to 3
Outputs:
- node_out: bfloat16 [32768, 256], P(('vert', 'feat'))
The draws below stay inside these ranges and needn't reach their ends.
Inputs may be any that keep to these rules, and one draw needn't show every extreme that they name: Row block r uses tile places 0 to tile_count[r] - 1; in every draw some row block uses all 16.
All inputs are finite; a program needn't handle non-finite values.
Results may differ from the reference program's by a relative error of at most 0.0044.
Values may be sent and summed in bfloat16 or wider, within the bound.
A program may use at most 128 MiB of HBM per device.

```python
import jax
import jax.numpy as jnp
from jax import lax

F = 256
BLK = 128
K = 16
SLOTS = 4
RB_DEV = 64
NRB = 256
NV = 32768
N_VERT = 4


def draw_tile_count(key, part):
    total = RB_DEV * N_VERT
    row_index = jnp.arange(total, dtype=jnp.int32)
    rank = row_index // RB_DEV
    ceiling = 1 + (K - 1) * (rank + 1) // N_VERT
    picks = jax.random.randint(key, (total,), 0, 1 << 20)
    counts = 1 + picks % ceiling
    chosen = jax.random.randint(jax.random.fold_in(key, 7), (), 0, total)
    return jnp.where(row_index == chosen, K, counts).astype(jnp.int32)


def with_ends(values, rng, least, top_value):
    spot = [jax.random.randint(jax.random.fold_in(rng, axis), (), 0, length) for axis, length in enumerate(values.shape)]
    longest = values.shape.index(max(values.shape))
    next_to = spot[:longest] + [(spot[longest] + 1) % values.shape[longest]] + spot[longest + 1:]
    return values.at[tuple(spot)].set(least).at[tuple(next_to)].set(top_value)


def block_levels(stream_key, dims, split, smallest, top_value):
    gain, own = 1.0, jax.random.fold_in(stream_key, 6)
    for dim, parts in split:
        steps = jnp.exp(jax.random.uniform(jax.random.fold_in(own, dim), (parts,), jnp.float32, smallest / len(split), top_value / len(split)))
        gain = gain * jnp.repeat(steps, dims[dim] // parts).reshape([-1 if axis == dim else 1 for axis in range(len(dims))])
    return gain


def scatter_about(rng, shape, width, reach, cuts=(), held_as=jnp.bfloat16):
    array = jax.random.normal(rng, shape, jnp.float32) * width
    if len(cuts) > 0:
        array = block_levels(rng, shape, cuts, -0.22, 0.18) * array
    return jnp.clip(array, min=-reach, max=reach).astype(held_as)


def setup_inputs(seed: int = 0) -> dict:
    streams_of = jax.random.split(jax.random.key(seed), 8)
    features = scatter_about(streams_of[0], (NV, F), 1.0, 6.0, ((0, 4), (1, 8)))
    tiles = scatter_about(streams_of[1], (NRB, K, BLK, BLK), (BLK * K // 2) ** -0.5, 0.1875, ((0, 4),))
    tile_cols = with_ends(jax.random.randint(streams_of[2], (NRB, K), 0, RB_DEV + N_VERT * SLOTS), jax.random.fold_in(streams_of[2], 1), 0, (RB_DEV + N_VERT * SLOTS) - 1).astype(jnp.int32)
    tile_count = draw_tile_count(jax.random.fold_in(streams_of[7], 71), 0)
    send_list = with_ends(jax.random.randint(streams_of[4], (N_VERT, N_VERT, SLOTS), 0, RB_DEV), jax.random.fold_in(streams_of[4], 1), 0, RB_DEV - 1).astype(jnp.int32)
    weight = scatter_about(streams_of[5], (F, F), F ** -0.5, 0.375)
    bias = scatter_about(streams_of[6], (F,), 0.5, 3.0, (), jnp.float32)
    return dict(features=features, tiles=tiles, tile_cols=tile_cols, tile_count=tile_count, send_list=send_list, weight=weight, bias=bias)


def reference(features, tiles, tile_cols, tile_count, send_list, weight, bias):
    row_owner = jnp.arange(RB_DEV * N_VERT, dtype=jnp.int32) // RB_DEV
    is_local = tile_cols < RB_DEV
    halo_slot = jnp.maximum(tile_cols - RB_DEV, 0)
    source = (halo_slot // SLOTS).astype(jnp.int32)
    position = (halo_slot % SLOTS).astype(jnp.int32)
    sent_block = send_list[source, row_owner[:, None], position]
    column = jnp.where(is_local, row_owner[:, None] * RB_DEV + tile_cols, source * RB_DEV + sent_block).astype(jnp.int32)
    blocks = features.reshape(RB_DEV * N_VERT, BLK, F)
    is_live = jnp.arange(K, dtype=jnp.int32)[None, :] < tile_count[:, None]

    def one_block(block_item):
        tile_row, col_row, live_row = block_item
        picked = blocks[col_row].astype(jnp.float32)
        products = jnp.einsum("kij,kjc->kic", tile_row.astype(jnp.float32), picked)
        kept = jnp.where(live_row[:, None, None], products, jnp.float32(0.0))
        return jnp.sum(kept, axis=0).astype(jnp.bfloat16)

    aggregated = lax.map(one_block, (tiles, column, is_live)).reshape(RB_DEV * N_VERT * BLK, F)
    mixed_rows = jnp.dot(aggregated, weight, preferred_element_type=jnp.float32) + bias
    return jnp.maximum(mixed_rows, jnp.float32(0.0)).astype(jnp.bfloat16)
```

```python
import functools

import jax
import jax.numpy as jnp
from jax import lax
from jax.experimental import pallas as pl
from jax.experimental.pallas import tpu as pltpu
from jax.sharding import PartitionSpec as P

MESH = pl.DeviceIdType.MESH
GROUP = 4
WINDOW = 6


def flipped(index, mask, count):
    total = 0
    bit = 1
    while bit < count:
        total = total + bit * ((index // bit + mask // bit) % 2)
        bit *= 2
    return total


def exchange_kernel(
    dims, cols, send, features, tiles, gathered,
    extended, local, outgoing, hidden, pages,
    load_sem, page_sem, halo_send, halo_recv, full_send, full_recv,
):
    verts, feats, blocks, depth, edge, width, slots, group, window = dims
    per_dest = blocks // feats
    parts = per_dest // group
    chunks = feats * parts
    span = group * edge
    vert = lax.axis_index("vert")
    feat = lax.axis_index("feat")

    def dest_of(chunk):
        return flipped(feat, feats - 1 - chunk // parts, feats)

    def page_copy(chunk):
        first = dest_of(chunk) * per_dest + (chunk % parts) * group
        slot = chunk % window
        return pltpu.make_async_copy(
            tiles.at[pl.ds(first, group)], pages.at[slot], page_sem.at[slot]
        )

    local_copy = pltpu.make_async_copy(features, local, load_sem)
    local_copy.start()
    for chunk in range(window):
        page_copy(chunk).start()
    extended[blocks + verts * slots] = jnp.zeros((width, edge), jnp.bfloat16)
    local_copy.wait()
    for block in range(blocks):
        extended[block] = local[:, pl.ds(block * edge, edge)]
    for step in range(verts):
        peer = (vert + step) % verts
        for slot in range(slots):
            outgoing[step, slot] = extended[send[peer * slots + slot]]
    barrier = pltpu.get_barrier_semaphore()
    for step in range(1, verts):
        pl.semaphore_signal(
            barrier, inc=1, device_id=((vert + step) % verts, feat), device_id_type=MESH
        )
    for step in range(1, feats):
        pl.semaphore_signal(
            barrier, inc=1, device_id=(vert, (feat + step) % feats), device_id_type=MESH
        )
    own_halo = pl.ds(blocks + vert * slots, slots)
    pl.semaphore_wait(barrier, verts + feats - 2)
    halos = []
    for step in range(1, verts):
        halo = pltpu.make_async_remote_copy(
            src_ref=outgoing.at[step],
            dst_ref=extended.at[own_halo],
            send_sem=halo_send.at[step],
            recv_sem=halo_recv.at[step],
            device_id=((vert + step) % verts, feat),
            device_id_type=MESH,
        )
        halo.start()
        halos.append(halo)
    extended[own_halo] = outgoing[0]
    for halo in halos:
        halo.wait()

    def outputs_of(chunk):
        at = pl.multiple_of((chunk % parts) * span, edge)
        return (
            hidden.at[chunk // parts, :, pl.ds(at, span)],
            gathered.at[pl.ds(pl.multiple_of(feat * width, width), width), pl.ds(at, span)],
        )

    def full_copy(chunk):
        source, target = outputs_of(chunk)
        return pltpu.make_async_remote_copy(
            src_ref=source,
            dst_ref=target,
            send_sem=full_send.at[chunk],
            recv_sem=full_recv.at[chunk],
            device_id=(vert, dest_of(chunk)),
            device_id_type=MESH,
        )

    def aggregate(chunk, carry):
        page_copy(chunk).wait()
        slot = chunk % window
        first = dest_of(chunk) * per_dest + (chunk % parts) * group
        for row in range(group):
            picked = []
            for place in range(depth):
                picked.append(extended[cols[(first + row) * depth + place]])
            page = jnp.concatenate([pages[slot, row, place] for place in range(depth)], axis=1)
            total = lax.dot_general(
                page,
                jnp.concatenate(picked, axis=1),
                (((1,), (1,)), ((), ())),
                preferred_element_type=jnp.float32,
            )
            at = pl.multiple_of((chunk % parts) * span + row * edge, edge)
            hidden[chunk // parts, :, pl.ds(at, edge)] = total.T.astype(jnp.bfloat16)

        @pl.when(chunk + window < chunks)
        def _():
            page_copy(chunk + window).start()

        @pl.when(chunk < chunks - parts)
        def _():
            full_copy(chunk).start()

        return carry

    lax.fori_loop(0, chunks, aggregate, 0)
    gathered[pl.ds(pl.multiple_of(feat * width, width), width), :] = hidden[feats - 1]

    def finish(chunk, carry):
        full_copy(chunk).wait()
        return carry

    lax.fori_loop(0, chunks - parts, finish, 0)


def per_device(features, tiles, tile_cols, tile_count, send_list, weight, bias):
    blocks, depth, edge = tiles.shape[:3]
    width = features.shape[1]
    verts, feats = lax.axis_size("vert"), lax.axis_size("feat")
    slots = send_list.shape[2]
    per_dest = blocks // feats
    group = min(GROUP, per_dest)
    chunks = blocks // group
    window = min(WINDOW, chunks)
    rows = per_dest * edge
    dead = blocks + verts * slots
    is_live = jnp.arange(depth, dtype=jnp.int32)[None, :] < tile_count[:, None]
    cols = jnp.where(is_live, tile_cols, dead).reshape(-1)
    dims = (verts, feats, blocks, depth, edge, width, slots, group, window)
    gathered = pl.pallas_call(
        functools.partial(exchange_kernel, dims),
        out_shape=jax.ShapeDtypeStruct((feats * width, rows), jnp.bfloat16),
        in_specs=[
            pl.BlockSpec(memory_space=pltpu.SMEM),
            pl.BlockSpec(memory_space=pltpu.SMEM),
            pl.BlockSpec(memory_space=pl.ANY),
            pl.BlockSpec(memory_space=pl.ANY),
        ],
        out_specs=pl.BlockSpec(memory_space=pltpu.VMEM),
        scratch_shapes=[
            pltpu.VMEM((dead + 1, width, edge), jnp.bfloat16),
            pltpu.VMEM((width, blocks * edge), jnp.bfloat16),
            pltpu.VMEM((verts, slots, width, edge), jnp.bfloat16),
            pltpu.VMEM((feats, width, rows), jnp.bfloat16),
            pltpu.VMEM((window, group, depth, edge, edge), jnp.bfloat16),
            pltpu.SemaphoreType.DMA,
            pltpu.SemaphoreType.DMA((window,)),
            pltpu.SemaphoreType.DMA((verts,)),
            pltpu.SemaphoreType.DMA((verts,)),
            pltpu.SemaphoreType.DMA((chunks,)),
            pltpu.SemaphoreType.DMA((chunks,)),
        ],
        compiler_params=pltpu.CompilerParams(
            collective_id=0, has_side_effects=True, vmem_limit_bytes=60 * 1024 * 1024
        ),
    )(cols, send_list.reshape(-1), features.T, tiles)
    mixed_rows = lax.dot_general(
        gathered, weight, (((0,), (0,)), ((), ())), preferred_element_type=jnp.float32
    )
    return jnp.maximum(mixed_rows + bias, jnp.float32(0.0)).astype(jnp.bfloat16)


def solution(mesh):
    return jax.shard_map(
        per_device,
        mesh=mesh,
        in_specs=(
            P("vert", "feat"),
            P("vert", None, None, None),
            P("vert", None),
            P("vert"),
            P("vert", None, None),
            P(),
            P(),
        ),
        out_specs=P(("vert", "feat"), None),
        check_vma=False,
    )
```

```python
import functools

import jax
import jax.numpy as jnp
from jax import lax
from jax.experimental import pallas as pl
from jax.experimental.pallas import tpu as pltpu
from jax.sharding import PartitionSpec as P

MESH = pl.DeviceIdType.MESH
GROUP = 4
WINDOW = 16


def flipped(index, mask, count):
    total = 0
    bit = 1
    while bit < count:
        total = total + bit * ((index // bit + mask // bit) % 2)
        bit *= 2
    return total


def exchange_kernel(
    dims, cols, count, send, features, tiles, gathered,
    extended, local, outgoing, landed, hidden, pages,
    load_sem, page_sem, halo_send, halo_recv, full_send, full_recv,
):
    verts, feats, blocks, depth, edge, width, slots, group, window = dims
    per_dest = blocks // feats
    parts = per_dest // group
    chunks = feats * parts
    span = group * edge
    dead = blocks + verts * slots
    vert = lax.axis_index("vert")
    feat = lax.axis_index("feat")

    def dest_of(chunk):
        return flipped(feat, feats - 1 - chunk // parts, feats)

    def page_copy(chunk):
        first = dest_of(chunk) * per_dest + (chunk % parts) * group
        slot = chunk % window
        return pltpu.make_async_copy(
            tiles.at[pl.ds(first, group)], pages.at[slot], page_sem.at[slot]
        )

    local_copy = pltpu.make_async_copy(features, local, load_sem)
    local_copy.start()
    barrier = pltpu.get_barrier_semaphore()
    for step in range(1, verts):
        pl.semaphore_signal(
            barrier, inc=1, device_id=((vert + step) % verts, feat), device_id_type=MESH
        )
    for step in range(1, feats):
        pl.semaphore_signal(
            barrier, inc=1, device_id=(vert, (feat + step) % feats), device_id_type=MESH
        )
    for chunk in range(window):
        page_copy(chunk).start()
    extended[dead] = jnp.zeros((width, edge), jnp.bfloat16)
    local_copy.wait()
    for block in range(blocks):
        extended[block] = local[:, pl.ds(block * edge, edge)]
    for step in range(verts):
        peer = (vert + step) % verts
        for slot in range(slots):
            outgoing[step, slot] = extended[send[0, peer, slot]]
    pl.semaphore_wait(barrier, verts + feats - 2)
    halos = []
    for step in range(1, verts):
        halo = pltpu.make_async_remote_copy(
            src_ref=outgoing.at[step],
            dst_ref=landed.at[step],
            send_sem=halo_send.at[step],
            recv_sem=halo_recv.at[step],
            device_id=((vert + step) % verts, feat),
            device_id_type=MESH,
        )
        halo.start()
        halos.append(halo)
    extended[pl.ds(blocks + vert * slots, slots)] = outgoing[0]
    for step in range(1, verts):
        halos[step - 1].wait()
        source = (vert + verts - step) % verts
        extended[pl.ds(blocks + source * slots, slots)] = landed[step]

    def outputs_of(chunk):
        at = pl.multiple_of((chunk % parts) * span, edge)
        return (
            hidden.at[chunk // parts, :, pl.ds(at, span)],
            gathered.at[pl.ds(pl.multiple_of(feat * width, width), width), pl.ds(at, span)],
        )

    def full_copy(chunk):
        source, target = outputs_of(chunk)
        return pltpu.make_async_remote_copy(
            src_ref=source,
            dst_ref=target,
            send_sem=full_send.at[chunk],
            recv_sem=full_recv.at[chunk],
            device_id=(vert, dest_of(chunk)),
            device_id_type=MESH,
        )

    def aggregate(chunk, carry):
        page_copy(chunk).wait()
        slot = chunk % window
        first = dest_of(chunk) * per_dest + (chunk % parts) * group
        for row in range(group):
            picked = []
            live = count[first + row]
            for place in range(depth):
                column = jnp.where(place < live, cols[place, first + row], dead)
                picked.append(extended[column])
            page = jnp.concatenate([pages[slot, row, place] for place in range(depth)], axis=1)
            total = lax.dot_general(
                page,
                jnp.concatenate(picked, axis=1),
                (((1,), (1,)), ((), ())),
                preferred_element_type=jnp.float32,
            )
            at = pl.multiple_of((chunk % parts) * span + row * edge, edge)
            hidden[chunk // parts, :, pl.ds(at, edge)] = total.T.astype(jnp.bfloat16)

        @pl.when(chunk + window < chunks)
        def _():
            page_copy(chunk + window).start()

        @pl.when(chunk < chunks - parts)
        def _():
            full_copy(chunk).start()

        return carry

    lax.fori_loop(0, chunks, aggregate, 0)
    gathered[pl.ds(pl.multiple_of(feat * width, width), width), :] = hidden[feats - 1]

    def finish(chunk, carry):
        full_copy(chunk).wait()
        return carry

    lax.fori_loop(0, chunks - parts, finish, 0)


def per_device(features, tiles, tile_cols, tile_count, send_list, weight, bias):
    blocks, depth, edge = tiles.shape[:3]
    width = features.shape[1]
    verts, feats = lax.axis_size("vert"), lax.axis_size("feat")
    slots = send_list.shape[2]
    per_dest = blocks // feats
    group = min(GROUP, per_dest)
    chunks = blocks // group
    window = min(WINDOW, chunks)
    rows = per_dest * edge
    dead = blocks + verts * slots
    dims = (verts, feats, blocks, depth, edge, width, slots, group, window)
    gathered = pl.pallas_call(
        functools.partial(exchange_kernel, dims),
        out_shape=jax.ShapeDtypeStruct((feats * width, rows), jnp.bfloat16),
        in_specs=[
            pl.BlockSpec(memory_space=pltpu.SMEM),
            pl.BlockSpec(memory_space=pltpu.SMEM),
            pl.BlockSpec(memory_space=pltpu.SMEM),
            pl.BlockSpec(memory_space=pl.ANY),
            pl.BlockSpec(memory_space=pl.ANY),
        ],
        out_specs=pl.BlockSpec(memory_space=pltpu.VMEM),
        scratch_shapes=[
            pltpu.VMEM((dead + 1, width, edge), jnp.bfloat16),
            pltpu.VMEM((width, blocks * edge), jnp.bfloat16),
            pltpu.VMEM((verts, slots, width, edge), jnp.bfloat16),
            pltpu.VMEM((verts, slots, width, edge), jnp.bfloat16),
            pltpu.VMEM((feats, width, rows), jnp.bfloat16),
            pltpu.VMEM((window, group, depth, edge, edge), jnp.bfloat16),
            pltpu.SemaphoreType.DMA,
            pltpu.SemaphoreType.DMA((window,)),
            pltpu.SemaphoreType.DMA((verts,)),
            pltpu.SemaphoreType.DMA((verts,)),
            pltpu.SemaphoreType.DMA((chunks,)),
            pltpu.SemaphoreType.DMA((chunks,)),
        ],
        compiler_params=pltpu.CompilerParams(
            collective_id=0, has_side_effects=True, vmem_limit_bytes=60 * 1024 * 1024
        ),
    )(tile_cols.T, tile_count, send_list, features.T, tiles)
    mixed_rows = lax.dot_general(
        gathered, weight, (((0,), (0,)), ((), ())), preferred_element_type=jnp.float32
    )
    return jnp.maximum(mixed_rows + bias, jnp.float32(0.0)).astype(jnp.bfloat16)


def solution(mesh):
    return jax.shard_map(
        per_device,
        mesh=mesh,
        in_specs=(
            P("vert", "feat"),
            P("vert", None, None, None),
            P("vert", None),
            P("vert"),
            P("vert", None, None),
            P(),
            P(),
        ),
        out_specs=P(("vert", "feat"), None),
        check_vma=False,
    )
```

```python
import functools

import jax
import jax.numpy as jnp
from jax import lax
from jax.experimental import pallas as pl
from jax.experimental.pallas import tpu as pltpu
from jax.sharding import PartitionSpec as P

MESH = pl.DeviceIdType.MESH
GROUP = 4
WINDOW = 16


def flipped(index, mask, count):
    total = 0
    bit = 1
    while bit < count:
        total = total + bit * ((index // bit + mask // bit) % 2)
        bit *= 2
    return total


def exchange_kernel(
    dims, cols_in, count_in, send_in, features, tiles, gathered,
    cols, count, send, table_sem, extended, local, outgoing, landed, hidden, pages,
    load_sem, page_sem, halo_send, halo_recv, full_send, full_recv,
):
    verts, feats, blocks, depth, edge, width, slots, group, window = dims
    per_dest = blocks // feats
    parts = per_dest // group
    chunks = feats * parts
    span = group * edge
    dead = blocks + verts * slots
    vert = lax.axis_index("vert")
    feat = lax.axis_index("feat")

    def dest_of(chunk):
        return flipped(feat, feats - 1 - chunk // parts, feats)

    def page_copy(chunk):
        first = dest_of(chunk) * per_dest + (chunk % parts) * group
        slot = chunk % window
        return pltpu.make_async_copy(
            tiles.at[pl.ds(first, group)], pages.at[slot], page_sem.at[slot]
        )

    local_copy = pltpu.make_async_copy(features, local, load_sem)
    local_copy.start()
    tables = [
        pltpu.make_async_copy(source, target, table_sem.at[at])
        for at, (source, target) in enumerate(((send_in, send), (cols_in, cols), (count_in, count)))
    ]
    for table in tables:
        table.start()
    barrier = pltpu.get_barrier_semaphore()
    for step in range(1, verts):
        pl.semaphore_signal(
            barrier, inc=1, device_id=((vert + step) % verts, feat), device_id_type=MESH
        )
    for step in range(1, feats):
        pl.semaphore_signal(
            barrier, inc=1, device_id=(vert, (feat + step) % feats), device_id_type=MESH
        )
    for chunk in range(window):
        page_copy(chunk).start()
    extended[dead] = jnp.zeros((width, edge), jnp.bfloat16)
    local_copy.wait()
    for table in tables:
        table.wait()
    for block in range(blocks):
        extended[block] = local[:, pl.ds(block * edge, edge)]
    for step in range(verts):
        peer = (vert + step) % verts
        for slot in range(slots):
            outgoing[step, slot] = extended[send[0, peer, slot]]
    pl.semaphore_wait(barrier, verts + feats - 2)
    halos = []
    for step in range(1, verts):
        halo = pltpu.make_async_remote_copy(
            src_ref=outgoing.at[step],
            dst_ref=landed.at[step],
            send_sem=halo_send.at[step],
            recv_sem=halo_recv.at[step],
            device_id=((vert + step) % verts, feat),
            device_id_type=MESH,
        )
        halo.start()
        halos.append(halo)
    extended[pl.ds(blocks + vert * slots, slots)] = outgoing[0]
    for step in range(1, verts):
        halos[step - 1].wait()
        source = (vert + verts - step) % verts
        extended[pl.ds(blocks + source * slots, slots)] = landed[step]

    def outputs_of(chunk):
        at = pl.multiple_of((chunk % parts) * span, edge)
        return (
            hidden.at[chunk // parts, :, pl.ds(at, span)],
            gathered.at[pl.ds(pl.multiple_of(feat * width, width), width), pl.ds(at, span)],
        )

    def full_copy(chunk):
        source, target = outputs_of(chunk)
        return pltpu.make_async_remote_copy(
            src_ref=source,
            dst_ref=target,
            send_sem=full_send.at[chunk],
            recv_sem=full_recv.at[chunk],
            device_id=(vert, dest_of(chunk)),
            device_id_type=MESH,
        )

    def aggregate(chunk, carry):
        page_copy(chunk).wait()
        slot = chunk % window
        first = dest_of(chunk) * per_dest + (chunk % parts) * group
        for row in range(group):
            picked = []
            live = count[first + row]
            for place in range(depth):
                column = jnp.where(place < live, cols[place, first + row], dead)
                picked.append(extended[column])
            page = jnp.concatenate([pages[slot, row, place] for place in range(depth)], axis=1)
            total = lax.dot_general(
                page,
                jnp.concatenate(picked, axis=1),
                (((1,), (1,)), ((), ())),
                preferred_element_type=jnp.float32,
            )
            at = pl.multiple_of((chunk % parts) * span + row * edge, edge)
            hidden[chunk // parts, :, pl.ds(at, edge)] = total.T.astype(jnp.bfloat16)

        @pl.when(chunk + window < chunks)
        def _():
            page_copy(chunk + window).start()

        @pl.when(chunk < chunks - parts)
        def _():
            full_copy(chunk).start()

        return carry

    lax.fori_loop(0, chunks, aggregate, 0)
    gathered[pl.ds(pl.multiple_of(feat * width, width), width), :] = hidden[feats - 1]

    def finish(chunk, carry):
        full_copy(chunk).wait()
        return carry

    lax.fori_loop(0, chunks - parts, finish, 0)


def per_device(features, tiles, tile_cols, tile_count, send_list, weight, bias):
    blocks, depth, edge = tiles.shape[:3]
    width = features.shape[1]
    verts, feats = lax.axis_size("vert"), lax.axis_size("feat")
    slots = send_list.shape[2]
    per_dest = blocks // feats
    group = min(GROUP, per_dest)
    chunks = blocks // group
    window = min(WINDOW, chunks)
    rows = per_dest * edge
    dead = blocks + verts * slots
    dims = (verts, feats, blocks, depth, edge, width, slots, group, window)
    gathered = pl.pallas_call(
        functools.partial(exchange_kernel, dims),
        out_shape=jax.ShapeDtypeStruct((feats * width, rows), jnp.bfloat16),
        in_specs=[
            pl.BlockSpec(memory_space=pltpu.HBM),
            pl.BlockSpec(memory_space=pltpu.HBM),
            pl.BlockSpec(memory_space=pltpu.HBM),
            pl.BlockSpec(memory_space=pltpu.HBM),
            pl.BlockSpec(memory_space=pltpu.HBM),
        ],
        out_specs=pl.BlockSpec(memory_space=pltpu.VMEM),
        scratch_shapes=[
            pltpu.SMEM((depth, blocks), jnp.int32),
            pltpu.SMEM((blocks,), jnp.int32),
            pltpu.SMEM(send_list.shape, jnp.int32),
            pltpu.SemaphoreType.DMA((3,)),
            pltpu.VMEM((dead + 1, width, edge), jnp.bfloat16),
            pltpu.VMEM((width, blocks * edge), jnp.bfloat16),
            pltpu.VMEM((verts, slots, width, edge), jnp.bfloat16),
            pltpu.VMEM((verts, slots, width, edge), jnp.bfloat16),
            pltpu.VMEM((feats, width, rows), jnp.bfloat16),
            pltpu.VMEM((window, group, depth, edge, edge), jnp.bfloat16),
            pltpu.SemaphoreType.DMA,
            pltpu.SemaphoreType.DMA((window,)),
            pltpu.SemaphoreType.DMA((verts,)),
            pltpu.SemaphoreType.DMA((verts,)),
            pltpu.SemaphoreType.DMA((chunks,)),
            pltpu.SemaphoreType.DMA((chunks,)),
        ],
        compiler_params=pltpu.CompilerParams(
            collective_id=0, has_side_effects=True, vmem_limit_bytes=60 * 1024 * 1024
        ),
    )(tile_cols.T, tile_count, send_list, features.T, tiles)
    mixed_rows = lax.dot_general(
        gathered, weight, (((0,), (0,)), ((), ())), preferred_element_type=jnp.float32
    )
    return jnp.maximum(mixed_rows + bias, jnp.float32(0.0)).astype(jnp.bfloat16)


def solution(mesh):
    return jax.shard_map(
        per_device,
        mesh=mesh,
        in_specs=(
            P("vert", "feat"),
            P("vert", None, None, None),
            P("vert", None),
            P("vert"),
            P("vert", None, None),
            P(),
            P(),
        ),
        out_specs=P(("vert", "feat"), None),
        check_vma=False,
    )
```
